32 devices in a mesh: agents: 8 (over z, x), group: 4 (over y, core).
Axes of the slice: x: 2, y: 2, z: 4, core: 2. Of those that a mesh axis runs over, the one named last changes fastest.
Arguments:
- q_lin: float32 [4, 40, 2048], P('group', None, 'agents'), may hold values from -6 to 6
- inverse: bfloat16 [4, 40, 40, 2048], P('group', None, None, 'agents'), may hold values from -0.5 to 1, as said below
- predict: bfloat16 [4, 40, 40, 2048], P('group', None, None, 'agents'), may hold values from -1 to 1
- free_traj: float32 [4, 40, 2048], P('group', None, 'agents'), may hold values from -6 to 6
- offsets: float32 [4, 8, 40, 2048], P('group', None, None, 'agents'), may hold values from -4 to 4
- multipliers: float32 [4, 8, 40, 2048], P('group', None, None, 'agents'), may hold values from -4 to 4
- nbr_owner: int32 [4, 8, 2048], P('group', None, 'agents'), may hold values from 0 to 7, as said below
- nbr_slot: int32 [4, 8, 2048], P('group', None, 'agents'), may hold values from -1 to 255
- platoon: int32 [4, 2048], P('group', 'agents'), may hold values from 0 to 127, as said below
Outputs:
- inputs_plan: float32 [4, 40, 2048], P('group', None, 'agents')
- multipliers_out: float32 [4, 8, 40, 2048], P('group', None, None, 'agents')
The draws below stay inside these ranges and needn't reach their ends.
Inputs may be any that keep to these rules, and one draw needn't show every extreme that they name: `nbr_owner`: an agent's own block index is its row in the region // 256; each neighbour's owner lies within 2 blocks of it, slot 0 is never padded. `inverse`: symmetric for every agent. `platoon`: 32 or more platoons hold no agent of any region.
All inputs are finite; a program needn't handle non-finite values. Where the reference program divides by a largest or mean magnitude, that divisor is 1e-20 or more.
Results may differ from the reference program's by a relative error of at most 0.0003.
Values sent between devices are 32-bit elements; how exact they have to be, the bound alone decides.
A program may use at most 64 MiB of HBM per device.

```python
import jax
import jax.numpy as jnp
from jax import lax

A_DEV = 256
QP = 40
TRAJ = 40
DEGREE = 8
SPAN = 2
NPLAT = 128
ITERS = 3
REGIONS = 4
PER = 2048


def neighbour_table(key):
    first, second, third = jax.random.split(jax.random.fold_in(key, 7), 3)
    shape = (REGIONS, DEGREE, PER)
    own = (jnp.arange(PER, dtype=jnp.int32) // A_DEV)[None, None, :]
    step = jax.random.randint(first, shape, -SPAN, SPAN + 1, dtype=jnp.int32)
    owner = jnp.clip(own + step, 0, PER // A_DEV - 1)
    slot = jax.random.randint(second, shape, 0, A_DEV, dtype=jnp.int32)
    alive = jax.random.randint(third, shape, 0, 4, dtype=jnp.int32) > 0
    alive = alive.at[:, 0, :].set(True)
    owner = jnp.where(alive, owner, own + jnp.zeros(shape, jnp.int32))
    slot = jnp.where(alive, slot, -1)
    return (owner, slot)


def draw_nbr_owner(key, part):
    return neighbour_table(key)[0]


def draw_nbr_slot(key, part):
    return neighbour_table(key)[1]


def draw_platoon(key, part):
    order_key, pick_key = jax.random.split(jax.random.fold_in(key, 13))
    order = jax.random.permutation(order_key, NPLAT).astype(jnp.int32)
    used = NPLAT - NPLAT // 4
    index = jax.random.randint(pick_key, (REGIONS, PER), 0, used, dtype=jnp.int32)
    return order[index].astype(jnp.int32)


def draw_inverse(key, part):
    noise_key = jax.random.fold_in(jax.random.fold_in(key, 11), 0)
    base = jax.random.normal(noise_key, (REGIONS, QP, QP, PER), jnp.float32) * 0.07
    sym = 0.5 * (base + jnp.transpose(base, (0, 2, 1, 3)))
    eye = jnp.eye(QP, dtype=jnp.float32)[None, :, :, None]
    whole = 0.5 * eye + sym
    return jnp.clip(whole, -0.5, 1.0).astype(jnp.bfloat16)


def levels(rng, extent, cuts, least, top_value):
    level, own = 1.0, jax.random.fold_in(rng, 6)
    for position, parts in cuts:
        heights = jnp.exp(jax.random.uniform(jax.random.fold_in(own, position), (parts,), jnp.float32, least / len(cuts), top_value / len(cuts)))
        level = level * jnp.repeat(heights, extent[position] // parts).reshape([-1 if axis == position else 1 for axis in range(len(extent))])
    return level


def scatter_about(own_key, extent, spread, most, shards=(), held_as=jnp.bfloat16):
    values = jax.random.normal(own_key, extent, jnp.float32) * spread
    if len(shards) > 0:
        values = levels(own_key, extent, shards, -0.22, 0.18) * values
    return jnp.clip(values, min=-most, max=most).astype(held_as)


def setup_inputs(seed: int = 0) -> dict:
    arg_keys = jax.random.split(jax.random.key(seed), 10)
    q_lin = scatter_about(arg_keys[0], (REGIONS, QP, PER), 1.0, 6.0, ((0, 4), (2, 8)), jnp.float32)
    inverse = draw_inverse(jax.random.fold_in(arg_keys[9], 71), 0)
    predict = scatter_about(arg_keys[2], (REGIONS, TRAJ, QP, PER), QP ** -0.5, 1.0, ((0, 4), (3, 8)))
    free_traj = scatter_about(arg_keys[3], (REGIONS, TRAJ, PER), 1.0, 6.0, ((0, 4), (2, 8)), jnp.float32)
    offsets = scatter_about(arg_keys[4], (REGIONS, DEGREE, TRAJ, PER), 0.5, 4.0, ((0, 4), (3, 8)), jnp.float32)
    multipliers = scatter_about(arg_keys[5], (REGIONS, DEGREE, TRAJ, PER), 0.5, 4.0, ((0, 4), (3, 8)), jnp.float32)
    nbr_owner = draw_nbr_owner(jax.random.fold_in(arg_keys[9], 71), 0)
    nbr_slot = draw_nbr_slot(jax.random.fold_in(arg_keys[9], 71), 0)
    platoon = draw_platoon(jax.random.fold_in(arg_keys[9], 71), 0)
    return {"q_lin": q_lin, "inverse": inverse, "predict": predict, "free_traj": free_traj, "offsets": offsets, "multipliers": multipliers, "nbr_owner": nbr_owner, "nbr_slot": nbr_slot, "platoon": platoon}


RHO = 0.5
KAPPA = 0.5


def lookup(field, nbr_owner, nbr_slot):
    live = nbr_slot >= 0
    column = jnp.where(live, nbr_owner * A_DEV + nbr_slot, 0).astype(jnp.int32)

    def one_region(rows, cols):
        taken = jnp.take(rows, cols.reshape(-1), axis=1)
        return taken.reshape(rows.shape[0], cols.shape[0], cols.shape[1])

    near = jax.vmap(one_region)(field, column)
    near = jnp.transpose(near, (0, 2, 1, 3))
    return near * live[:, :, None, :].astype(jnp.float32)


def platoon_pull(field, onehot):
    sums = jnp.einsum('rta,rpa->tp', field, onehot, precision=lax.Precision.HIGHEST)
    counts = jnp.sum(onehot, axis=(0, 2))
    means = sums / jnp.maximum(counts, 1.0)[None, :]
    return jnp.einsum('tp,rpa->rta', means, onehot, precision=lax.Precision.HIGHEST)


def reference(q_lin, inverse, predict, free_traj, offsets, multipliers, nbr_owner, nbr_slot, platoon):
    live = (nbr_slot >= 0).astype(jnp.float32)[:, :, None, :]
    onehot = (platoon[:, None, :] == jnp.arange(NPLAT, dtype=jnp.int32)[None, :, None]).astype(jnp.float32)
    inverse_wide = inverse.astype(jnp.float32)
    predict_wide = predict.astype(jnp.float32)
    traj = free_traj
    lam = multipliers
    near = lookup(traj, nbr_owner, nbr_slot)
    attract = platoon_pull(traj, onehot)
    plan = jnp.zeros_like(q_lin)
    for step in range(ITERS):
        coupling = jnp.sum(live * (lam - RHO * (near + offsets)), axis=1) - KAPPA * attract
        rhs = q_lin + jnp.einsum('rtja,rta->rja', predict_wide, coupling, precision=lax.Precision.HIGHEST)
        plan = -jnp.einsum('rija,rja->ria', inverse_wide, rhs, precision=lax.Precision.HIGHEST)
        traj = jnp.einsum('rtja,rja->rta', predict_wide, plan, precision=lax.Precision.HIGHEST) + free_traj
        near = lookup(traj, nbr_owner, nbr_slot)
        gap = live * (traj[:, None] - near - offsets)
        peak = jnp.max(jnp.abs(gap))
        lam = lam + gap / (1.0 + peak)
        if step + 1 < ITERS:
            attract = platoon_pull(traj, onehot)
    return plan, lam
```

```python
import functools

import jax
import jax.numpy as jnp
from jax import lax
from jax.experimental import pallas as pl
from jax.experimental.pallas import tpu as pltpu
from jax.sharding import PartitionSpec as P

SPAN = 2
NPLAT = 128
ITERS = 3
RHO = 0.5
KAPPA = 0.5
LANES = 128
F32 = jnp.float32
BF16 = jnp.bfloat16
MESH = pl.DeviceIdType.MESH


def split(value):
    high = value.astype(BF16)
    low = (value - high.astype(F32)).astype(BF16)
    return high, low


def kernel(
    agents, group, fold,
    q_hbm, inv_hbm, pre_hbm, free_hbm, off_hbm, mul_hbm, owner_hbm, slot_hbm, plat_hbm,
    plan_hbm, lam_hbm,
    q, inv, pre, off, lam, owner, slot, plat,
    plan, gap, coup, rhs, traj, near_in,
    rs_out, rs_in, line_out, line_in, ag_out, ag_in, peak_out, peak_in, top_out, top_in,
    inv_count, lane_tab, tile_tab,
    load_sem, store_sem,
    near_send, near_recv, rs_send, rs_recv, line_send, line_recv, ag_send, ag_recv,
    peak_send, peak_recv, top_send, top_recv,
):
    me = lax.axis_index("agents")
    mine = lax.axis_index("group")
    lines = agents // fold
    plane = fold * group
    high, low = me // fold, me % fold
    spot = low * group + mine
    rows, block = q.shape
    degree = slot.shape[0]
    halves = block // LANES
    part = -(-rows // plane)

    loads = {}
    for number, (name, source, target) in enumerate((
        ("free", free_hbm, traj.at[0]), ("plat", plat_hbm, plat), ("slot", slot_hbm, slot),
        ("owner", owner_hbm, owner), ("q", q_hbm, q), ("lam", mul_hbm, lam), ("off", off_hbm, off),
        ("pre", pre_hbm, pre), ("inv", inv_hbm, inv),
    )):
        loads[name] = pltpu.make_async_copy(source, target, load_sem.at[number])
        loads[name].start()

    def plane_peer(offset):
        other = lax.rem(spot + offset, plane)
        return other, {"agents": high * fold + other // group, "group": lax.rem(other, group)}

    def line_peer(offset):
        return {"agents": lax.rem(high + offset, lines) * fold + low, "group": mine}

    def exists(step):
        return jnp.logical_and(me + step >= 0, me + step < agents)

    steps = [d for d in range(-SPAN, SPAN + 1) if d != 0]
    barrier = pltpu.get_barrier_semaphore()
    for offset in range(1, plane):
        pl.semaphore_signal(barrier, inc=1, device_id=plane_peer(offset)[1], device_id_type=MESH)
    for offset in range(1, lines):
        pl.semaphore_signal(barrier, inc=1, device_id=line_peer(offset), device_id_type=MESH)
    expected = plane - 1 + lines - 1
    for step in steps:
        @pl.when(exists(step))
        def _():
            pl.semaphore_signal(
                barrier, inc=1, device_id={"agents": me + step, "group": mine}, device_id_type=MESH
            )
        expected = expected + jnp.where(exists(step), 1, 0)

    def near_copy(turn, step):
        return pltpu.make_async_remote_copy(
            src_ref=traj.at[turn], dst_ref=near_in.at[turn, SPAN - step],
            send_sem=near_send.at[turn, SPAN + step], recv_sem=near_recv.at[turn, SPAN - step],
            device_id={"agents": me + step, "group": mine}, device_id_type=MESH)

    def near_arrival(turn, step):
        return pltpu.make_async_remote_copy(
            src_ref=traj.at[turn], dst_ref=near_in.at[turn, SPAN + step],
            send_sem=near_send.at[turn, SPAN + step], recv_sem=near_recv.at[turn, SPAN + step],
            device_id={"agents": me + step, "group": mine}, device_id_type=MESH)

    def rs_copy(turn, offset):
        other, device = plane_peer(offset)
        return pltpu.make_async_remote_copy(
            src_ref=rs_out.at[turn, other], dst_ref=rs_in.at[turn, offset],
            send_sem=rs_send.at[turn, offset], recv_sem=rs_recv.at[turn, offset],
            device_id=device, device_id_type=MESH)

    def line_copy(turn, offset):
        return pltpu.make_async_remote_copy(
            src_ref=line_out.at[turn], dst_ref=line_in.at[turn, offset],
            send_sem=line_send.at[turn, offset], recv_sem=line_recv.at[turn, offset],
            device_id=line_peer(offset), device_id_type=MESH)

    def ag_copy(turn, offset):
        return pltpu.make_async_remote_copy(
            src_ref=ag_out.at[turn], dst_ref=ag_in.at[turn, spot],
            send_sem=ag_send.at[turn, offset], recv_sem=ag_recv.at[turn, offset],
            device_id=plane_peer(offset)[1], device_id_type=MESH)

    def ag_arrival(turn, offset):
        return pltpu.make_async_remote_copy(
            src_ref=ag_out.at[turn], dst_ref=ag_in.at[turn, lax.rem(spot + plane - offset, plane)],
            send_sem=ag_send.at[turn, offset], recv_sem=ag_recv.at[turn, offset],
            device_id=plane_peer(offset)[1], device_id_type=MESH)

    def peak_copy(turn, offset):
        return pltpu.make_async_remote_copy(
            src_ref=peak_out.at[turn], dst_ref=peak_in.at[turn, offset],
            send_sem=peak_send.at[turn, offset], recv_sem=peak_recv.at[turn, offset],
            device_id=line_peer(offset), device_id_type=MESH)

    def top_copy(turn, offset):
        return pltpu.make_async_remote_copy(
            src_ref=top_out.at[turn], dst_ref=top_in.at[turn, offset],
            send_sem=top_send.at[turn, offset], recv_sem=top_recv.at[turn, offset],
            device_id=plane_peer(offset)[1], device_id_type=MESH)

    def onehot():
        names = lax.broadcasted_iota(jnp.int32, (NPLAT, block), 0)
        return jnp.where(names == plat[...], 1.0, 0.0).astype(BF16)

    def platoon_sums(value):
        hot = onehot()
        dims = (((1,), (1,)), ((), ()))
        first, second = split(value)
        return lax.dot_general(first, hot, dims, preferred_element_type=F32) + lax.dot_general(
            second, hot, dims, preferred_element_type=F32)

    def start_platoon(turn):
        sums = platoon_sums(traj[turn])
        for piece in range(plane):
            begin, end = min(rows, piece * part), min(rows, (piece + 1) * part)
            if end > begin:
                rs_out[turn, piece, 0:end - begin, :] = sums[begin:end, :]
            if turn == 0:
                ones = jnp.ones((16, block), BF16)
                if piece == 0:
                    counts = lax.dot_general(
                        ones, onehot(), (((1,), (1,)), ((), ())), preferred_element_type=F32)[0:1]
                rs_out[turn, piece, part:part + 1, :] = counts
        for offset in range(1, plane):
            rs_copy(turn, offset).start()

    def middle_platoon(turn):
        total = rs_out[turn, spot]
        for offset in range(1, plane):
            rs_copy(turn, offset).wait()
            total = total + rs_in[turn, offset]
        line_out[turn] = total
        for offset in range(1, lines):
            line_copy(turn, offset).start()

    def late_platoon(turn):
        total = line_out[turn]
        for offset in range(1, lines):
            line_copy(turn, offset).wait()
            total = total + line_in[turn, offset]
        if turn == 0:
            inv_count[...] = 1.0 / jnp.maximum(total[part:part + 1, :], 1.0)
        mean = total * inv_count[...]
        ag_out[turn] = mean
        for offset in range(1, plane):
            ag_copy(turn, offset).start()
        ag_in[turn, spot] = mean

    def finish_platoon(turn):
        for offset in range(1, plane):
            ag_copy(turn, offset).wait_send()
            ag_arrival(turn, offset).wait_recv()
        pieces = []
        for piece in range(plane):
            begin, end = min(rows, piece * part), min(rows, (piece + 1) * part)
            if end > begin:
                pieces.append(ag_in[turn, piece, 0:end - begin, :])
        means = jnp.concatenate(pieces, axis=0)
        hot = onehot()
        first, second = split(means)
        return jnp.dot(first, hot, preferred_element_type=F32) + jnp.dot(
            second, hot, preferred_element_type=F32)

    def start_near(turn):
        for step in steps:
            @pl.when(exists(step))
            def _():
                near_copy(turn, step).start()

    def wait_near(turn):
        for step in steps:
            @pl.when(exists(step))
            def _():
                near_copy(turn, step).wait_send()
                near_arrival(turn, step).wait_recv()

    def look(turn, slot_index, half):
        window = pl.ds(half * LANES, LANES)
        lane = lane_tab[slot_index, :, window]
        tile = tile_tab[slot_index, :, window]
        out = []
        for band in range(rows // 8):
            near = jnp.zeros((8, LANES), F32)
            for distance in range(2 * SPAN + 1):
                for side in range(halves):
                    span = (pl.ds(band * 8, 8), pl.ds(side * LANES, LANES))
                    if distance == SPAN:
                        source = traj[(turn,) + span]
                    else:
                        source = near_in[(turn, distance) + span]
                    taken = jnp.take_along_axis(source, lane, axis=1, mode="promise_in_bounds")
                    near = jnp.where(tile == distance * halves + side, taken, near)
            out.append(near)
        return tile >= 0, out

    def start_peak(turn, peak):
        peak_out[turn] = peak
        for offset in range(1, lines):
            peak_copy(turn, offset).start()

    def middle_peak(turn):
        peak = peak_out[turn]
        for offset in range(1, lines):
            peak_copy(turn, offset).wait()
            peak = jnp.maximum(peak, peak_in[turn, offset])
        top_out[turn] = peak
        for offset in range(1, plane):
            top_copy(turn, offset).start()

    def finish_peak(turn):
        peak = top_out[turn]
        for offset in range(1, plane):
            top_copy(turn, offset).wait()
            peak = jnp.maximum(peak, top_in[turn, offset])
        peak = jnp.max(jnp.max(peak, axis=0, keepdims=True), axis=1, keepdims=True)
        return 1.0 / (1.0 + peak)

    def tables():
        where = slot[...]
        tile = jnp.where(where >= 0, (owner[...] - me + SPAN) * halves + where // LANES, -1)
        lane = lax.rem(jnp.maximum(where, 0), LANES)
        for index in range(degree):
            lane_tab[index] = jnp.broadcast_to(lane[index:index + 1], (8, block))
            tile_tab[index] = jnp.broadcast_to(tile[index:index + 1], (8, block))

    def down(matrix, vector_ref, start):
        def body(band, total):
            rows8 = vector_ref[pl.ds(pl.multiple_of(band * 8, 8), 8), :]
            for index in range(8):
                total = total + matrix[band * 8 + index].astype(F32) * rows8[index:index + 1, :]
            return total
        return lax.fori_loop(0, rows // 8, body, start)

    loads["free"].wait()
    loads["plat"].wait()
    pl.semaphore_wait(barrier, expected)
    rs_out[...] = jnp.zeros_like(rs_out)
    start_platoon(0)
    start_near(0)
    for name in ("slot", "owner", "q", "lam", "off", "pre", "inv"):
        loads[name].wait()
    tables()
    middle_platoon(0)
    wait_near(0)
    late_platoon(0)

    coup[...] = jnp.zeros_like(coup)

    def first_body(index, carry):
        for half in range(halves):
            alive, near = look(0, index, half)
            for band in range(rows // 8):
                span = (pl.ds(band * 8, 8), pl.ds(half * LANES, LANES))
                term = lam[(index,) + span] - RHO * (near[band] + off[(index,) + span])
                coup[span] = coup[span] + jnp.where(alive, term, 0.0)
        return carry

    lax.fori_loop(0, degree, first_body, 0)

    for turn in range(ITERS):
        if turn > 0:
            factor = finish_peak(turn - 1)
            base = coup[...] + rhs[...] * factor
        else:
            base = coup[...]
        coup[...] = base - KAPPA * finish_platoon(turn)
        if turn > 0:
            lam[...] = lam[...] + gap[...] * factor[None]
        rhs[...] = down(pre, coup, q[...])
        plan[...] = -down(inv, rhs, jnp.zeros((rows, block), F32))
        current = plan[...]

        def up_body(band, carry):
            out = []
            for index in range(8):
                product = pre[band * 8 + index].astype(F32) * current
                out.append(jnp.sum(product, axis=0, keepdims=True))
            span = pl.ds(pl.multiple_of(band * 8, 8), 8)
            traj[turn + 1, span, :] = jnp.concatenate(out, axis=0) + traj[0, span, :]
            return carry

        lax.fori_loop(0, rows // 8, up_body, 0)
        more = turn + 1 < ITERS
        if more:
            start_platoon(turn + 1)
        start_near(turn + 1)
        if more:
            middle_platoon(turn + 1)
        wait_near(turn + 1)
        coup[...] = jnp.zeros_like(coup)
        rhs[...] = jnp.zeros_like(rhs)

        def body(index, peak):
            for half in range(halves):
                alive, near = look(turn + 1, index, half)
                for band in range(rows // 8):
                    span = (pl.ds(band * 8, 8), pl.ds(half * LANES, LANES))
                    wish = near[band] + off[(index,) + span]
                    miss = jnp.where(alive, traj[(turn + 1,) + span] - wish, 0.0)
                    gap[(index,) + span] = miss
                    peak = jnp.maximum(peak, jnp.abs(miss))
                    if more:
                        term = lam[(index,) + span] - RHO * wish
                        coup[span] = coup[span] + jnp.where(alive, term, 0.0)
                        rhs[span] = rhs[span] + miss
            return peak

        peak = lax.fori_loop(0, degree, body, jnp.zeros((8, LANES), F32))
        start_peak(turn, peak)
        if more:
            late_platoon(turn + 1)
        else:
            done_plan = pltpu.make_async_copy(plan, plan_hbm, store_sem.at[0])
            done_plan.start()
        middle_peak(turn)

    factor = finish_peak(ITERS - 1)
    lam[...] = lam[...] + gap[...] * factor[None]
    done_lam = pltpu.make_async_copy(lam, lam_hbm, store_sem.at[1])
    done_lam.start()
    done_plan.wait()
    done_lam.wait()


def local(agents, group, q_lin, inverse, predict, free_traj, offsets, multipliers, nbr_owner, nbr_slot, platoon):
    rows, block = q_lin.shape[1:]
    degree = nbr_slot.shape[1]
    fold = 2 if agents % 2 == 0 else 1
    lines, plane = agents // fold, fold * group
    part = -(-rows // plane)
    tile = (-(-(part + 1) // 8) * 8, NPLAT)
    turns = ITERS
    wide = 2 * SPAN + 1
    dma = lambda *shape: pltpu.SemaphoreType.DMA(shape)
    vmem = lambda *shape: pltpu.VMEM(shape, F32)
    anywhere = pl.BlockSpec(memory_space=pl.ANY)
    plan, lam = pl.pallas_call(
        functools.partial(kernel, agents, group, fold),
        out_shape=(
            jax.ShapeDtypeStruct((rows, block), F32),
            jax.ShapeDtypeStruct((degree, rows, block), F32),
        ),
        in_specs=[anywhere] * 9,
        out_specs=[anywhere] * 2,
        scratch_shapes=[
            vmem(rows, block),
            pltpu.VMEM((rows, rows, block), BF16),
            pltpu.VMEM((rows, rows, block), BF16),
            vmem(degree, rows, block),
            vmem(degree, rows, block),
            pltpu.VMEM((degree, block), jnp.int32),
            pltpu.VMEM((degree, block), jnp.int32),
            pltpu.VMEM((1, block), jnp.int32),
            vmem(rows, block),
            vmem(degree, rows, block),
            vmem(rows, block),
            vmem(rows, block),
            vmem(turns + 1, rows, block),
            vmem(turns + 1, wide, rows, block),
            vmem(turns, plane, *tile),
            vmem(turns, plane, *tile),
            vmem(turns, *tile),
            vmem(turns, lines, *tile),
            vmem(turns, *tile),
            vmem(turns, plane, *tile),
            vmem(turns, 8, LANES),
            vmem(turns, lines, 8, LANES),
            vmem(turns, 8, LANES),
            vmem(turns, plane, 8, LANES),
            vmem(1, NPLAT),
            pltpu.VMEM((degree, 8, block), jnp.int32),
            pltpu.VMEM((degree, 8, block), jnp.int32),
            dma(9), dma(2),
            dma(turns + 1, wide), dma(turns + 1, wide),
            dma(turns, plane), dma(turns, plane),
            dma(turns, lines), dma(turns, lines),
            dma(turns, plane), dma(turns, plane),
            dma(turns, lines), dma(turns, lines),
            dma(turns, plane), dma(turns, plane),
        ],
        compiler_params=pltpu.CompilerParams(collective_id=0, has_side_effects=True),
    )(
        q_lin[0], inverse[0], predict[0], free_traj[0], offsets[0], multipliers[0],
        nbr_owner[0], nbr_slot[0], platoon,
    )
    return plan[None], lam[None]


def solution(mesh):
    agents, group = mesh.shape["agents"], mesh.shape["group"]
    return jax.shard_map(
        functools.partial(local, agents, group),
        mesh=mesh,
        in_specs=(
            P("group", None, "agents"),
            P("group", None, None, "agents"),
            P("group", None, None, "agents"),
            P("group", None, "agents"),
            P("group", None, None, "agents"),
            P("group", None, None, "agents"),
            P("group", None, "agents"),
            P("group", None, "agents"),
            P("group", "agents"),
        ),
        out_specs=(P("group", None, "agents"), P("group", None, None, "agents")),
        check_vma=False,
    )
```

```python
import functools

import jax
import jax.numpy as jnp
from jax import lax
from jax.experimental import pallas as pl
from jax.experimental.pallas import tpu as pltpu
from jax.sharding import PartitionSpec as P

SPAN = 2
NPLAT = 128
ITERS = 3
RHO = 0.5
KAPPA = 0.5
LANES = 128
F32 = jnp.float32
BF16 = jnp.bfloat16
ORDER = 2
MESH = pl.DeviceIdType.MESH


def split(value):
    high = value.astype(BF16)
    low = (value - high.astype(F32)).astype(BF16)
    return high, low


def kernel(
    agents, group, fold,
    q_hbm, inv_hbm, pre_hbm, free_hbm, off_hbm, mul_hbm, owner_hbm, slot_hbm, plat_hbm,
    plan, lam, gap, scale,
    q, inv, pre, off, owner, slot, plat,
    coup, rhs, miss_sum, slope, plan_slope, traj, near_in,
    rs_out, rs_in, line_out, line_in, ag_out, ag_in, peak_out, peak_in,
    inv_count, lane_tab, tile_tab,
    load_sem,
    near_send, near_recv, rs_send, rs_recv, line_send, line_recv, ag_send, ag_recv,
    peak_send, peak_recv,
):
    me = lax.axis_index("agents")
    mine = lax.axis_index("group")
    lines = agents // fold
    plane = fold * group
    everyone = agents * group
    high, low = me // fold, me % fold
    spot = low * group + mine
    rows, block = q.shape
    degree = slot.shape[0]
    halves = block // LANES
    part = -(-rows // plane)

    loads = {}
    for number, (name, source, target) in enumerate((
        ("free", free_hbm, traj.at[0]), ("plat", plat_hbm, plat), ("slot", slot_hbm, slot),
        ("owner", owner_hbm, owner), ("q", q_hbm, q), ("lam", mul_hbm, lam), ("off", off_hbm, off),
        ("pre", pre_hbm, pre), ("inv", inv_hbm, inv),
    )):
        loads[name] = pltpu.make_async_copy(source, target, load_sem.at[number])
        loads[name].start()

    def plane_peer(offset):
        other = lax.rem(spot + offset, plane)
        return other, {"agents": high * fold + other // group, "group": lax.rem(other, group)}

    def line_peer(offset):
        return {"agents": lax.rem(high + offset, lines) * fold + low, "group": mine}

    def exists(step):
        return jnp.logical_and(me + step >= 0, me + step < agents)

    steps = [d for d in range(-SPAN, SPAN + 1) if d != 0]
    barrier = pltpu.get_barrier_semaphore()
    for offset in range(1, plane):
        pl.semaphore_signal(barrier, inc=1, device_id=plane_peer(offset)[1], device_id_type=MESH)
    for offset in range(1, lines):
        pl.semaphore_signal(barrier, inc=1, device_id=line_peer(offset), device_id_type=MESH)
    expected = plane - 1 + lines - 1
    for step in steps:
        @pl.when(exists(step))
        def _():
            pl.semaphore_signal(
                barrier, inc=1, device_id={"agents": me + step, "group": mine}, device_id_type=MESH
            )
        expected = expected + jnp.where(exists(step), 1, 0)

    def near_copy(turn, step):
        return pltpu.make_async_remote_copy(
            src_ref=traj.at[turn], dst_ref=near_in.at[turn, SPAN - step],
            send_sem=near_send.at[turn, SPAN + step], recv_sem=near_recv.at[turn, SPAN - step],
            device_id={"agents": me + step, "group": mine}, device_id_type=MESH)

    def near_arrival(turn, step):
        return pltpu.make_async_remote_copy(
            src_ref=traj.at[turn], dst_ref=near_in.at[turn, SPAN + step],
            send_sem=near_send.at[turn, SPAN + step], recv_sem=near_recv.at[turn, SPAN + step],
            device_id={"agents": me + step, "group": mine}, device_id_type=MESH)

    def rs_copy(turn, offset):
        other, device = plane_peer(offset)
        return pltpu.make_async_remote_copy(
            src_ref=rs_out.at[turn, other], dst_ref=rs_in.at[turn, offset],
            send_sem=rs_send.at[turn, offset], recv_sem=rs_recv.at[turn, offset],
            device_id=device, device_id_type=MESH)

    def line_copy(turn, offset):
        return pltpu.make_async_remote_copy(
            src_ref=line_out.at[turn], dst_ref=line_in.at[turn, offset],
            send_sem=line_send.at[turn, offset], recv_sem=line_recv.at[turn, offset],
            device_id=line_peer(offset), device_id_type=MESH)

    def ag_copy(turn, offset):
        return pltpu.make_async_remote_copy(
            src_ref=ag_out.at[turn], dst_ref=ag_in.at[turn, spot],
            send_sem=ag_send.at[turn, offset], recv_sem=ag_recv.at[turn, offset],
            device_id=plane_peer(offset)[1], device_id_type=MESH)

    def ag_arrival(turn, offset):
        return pltpu.make_async_remote_copy(
            src_ref=ag_out.at[turn], dst_ref=ag_in.at[turn, lax.rem(spot + plane - offset, plane)],
            send_sem=ag_send.at[turn, offset], recv_sem=ag_recv.at[turn, offset],
            device_id=plane_peer(offset)[1], device_id_type=MESH)

    def peak_copy(turn, offset):
        other = lax.rem(me * group + mine + offset, everyone)
        return pltpu.make_async_remote_copy(
            src_ref=peak_out.at[turn], dst_ref=peak_in.at[turn, offset],
            send_sem=peak_send.at[turn], recv_sem=peak_recv.at[turn],
            device_id={"agents": other // group, "group": lax.rem(other, group)},
            device_id_type=MESH)

    def onehot():
        names = lax.broadcasted_iota(jnp.int32, (NPLAT, block), 0)
        return jnp.where(names == plat[...], 1.0, 0.0).astype(BF16)

    def platoon_sums(value):
        hot = onehot()
        dims = (((1,), (1,)), ((), ()))
        first, second = split(value)
        return lax.dot_general(first, hot, dims, preferred_element_type=F32) + lax.dot_general(
            second, hot, dims, preferred_element_type=F32)

    def start_platoon(turn):
        sums = platoon_sums(traj[turn])
        for piece in range(plane):
            begin, end = min(rows, piece * part), min(rows, (piece + 1) * part)
            if end > begin:
                rs_out[turn, piece, 0:end - begin, :] = sums[begin:end, :]
            if turn == 0:
                ones = jnp.ones((16, block), BF16)
                if piece == 0:
                    counts = lax.dot_general(
                        ones, onehot(), (((1,), (1,)), ((), ())), preferred_element_type=F32)[0:1]
                rs_out[turn, piece, part:part + 1, :] = counts
        for offset in range(1, plane):
            rs_copy(turn, offset).start()

    def middle_platoon(turn):
        total = rs_out[turn, spot]
        for offset in range(1, plane):
            rs_copy(turn, offset).wait()
            total = total + rs_in[turn, offset]
        line_out[turn] = total
        for offset in range(1, lines):
            line_copy(turn, offset).start()

    def late_platoon(turn):
        total = line_out[turn]
        for offset in range(1, lines):
            line_copy(turn, offset).wait()
            total = total + line_in[turn, offset]
        if turn == 0:
            inv_count[...] = 1.0 / jnp.maximum(total[part:part + 1, :], 1.0)
        mean = total * inv_count[...]
        ag_out[turn] = mean
        for offset in range(1, plane):
            ag_copy(turn, offset).start()
        ag_in[turn, spot] = mean

    def finish_platoon(turn):
        for offset in range(1, plane):
            ag_copy(turn, offset).wait_send()
            ag_arrival(turn, offset).wait_recv()
        pieces = []
        for piece in range(plane):
            begin, end = min(rows, piece * part), min(rows, (piece + 1) * part)
            if end > begin:
                pieces.append(ag_in[turn, piece, 0:end - begin, :])
        means = jnp.concatenate(pieces, axis=0)
        hot = onehot()
        first, second = split(means)
        return jnp.dot(first, hot, preferred_element_type=F32) + jnp.dot(
            second, hot, preferred_element_type=F32)

    def start_near(turn, steps=steps):
        for step in steps:
            @pl.when(exists(step))
            def _():
                near_copy(turn, step).start()

    def wait_near(turn):
        for step in steps:
            @pl.when(exists(step))
            def _():
                near_copy(turn, step).wait_send()
                near_arrival(turn, step).wait_recv()

    def look(turn, slot_index, half):
        window = pl.ds(half * LANES, LANES)
        lane = lane_tab[slot_index, :, window]
        tile = tile_tab[slot_index, :, window]
        out = []
        for band in range(rows // 8):
            near = jnp.zeros((8, LANES), F32)
            for distance in range(2 * SPAN + 1):
                for side in range(halves):
                    span = (pl.ds(band * 8, 8), pl.ds(side * LANES, LANES))
                    if distance == SPAN:
                        source = traj[(turn,) + span]
                    else:
                        source = near_in[(turn, distance) + span]
                    taken = jnp.take_along_axis(source, lane, axis=1, mode="promise_in_bounds")
                    near = jnp.where(tile == distance * halves + side, taken, near)
            out.append(near)
        return tile >= 0, out

    def start_peak(turn, peak):
        peak_out[turn] = jnp.max(peak, axis=0, keepdims=True)
        for offset in range(1, everyone):
            peak_copy(turn, offset).start()

    def finish_peak(turn):
        landed = peak_in.at[turn, pl.ds(1, everyone - 1)]
        pltpu.make_async_copy(landed, landed, peak_send.at[turn]).wait()
        pltpu.make_async_copy(landed, landed, peak_recv.at[turn]).wait()
        peak = peak_out[turn]
        for offset in range(1, everyone):
            peak = jnp.maximum(peak, peak_in[turn, offset])
        return 1.0 / (1.0 + jnp.max(peak, axis=1, keepdims=True))

    def tables():
        where = slot[...]
        tile = jnp.where(where >= 0, (owner[...] - me + SPAN) * halves + where // LANES, -1)
        lane = lax.rem(jnp.maximum(where, 0), LANES)
        for index in range(degree):
            lane_tab[index] = jnp.broadcast_to(lane[index:index + 1], (8, block))
            tile_tab[index] = jnp.broadcast_to(tile[index:index + 1], (8, block))

    def down(matrix, vector_ref, start):
        def body(band, total):
            rows8 = vector_ref[pl.ds(pl.multiple_of(band * 8, 8), 8), :]
            for index in range(8):
                total = total + matrix[band * 8 + index].astype(F32) * rows8[index:index + 1, :]
            return total
        return lax.fori_loop(0, rows // 8, body, start)

    loads["free"].wait()
    loads["plat"].wait()
    pl.semaphore_wait(barrier, expected)
    rs_out[...] = jnp.zeros_like(rs_out)
    start_platoon(0)
    start_near(0)
    for name in ("slot", "owner", "q", "lam", "off", "pre", "inv"):
        loads[name].wait()
    tables()
    middle_platoon(0)
    wait_near(0)
    late_platoon(0)

    coup[...] = jnp.zeros_like(coup)

    def first_body(index, carry):
        for half in range(halves):
            alive, near = look(0, index, half)
            for band in range(rows // 8):
                span = (pl.ds(band * 8, 8), pl.ds(half * LANES, LANES))
                term = lam[(index,) + span] - RHO * (near[band] + off[(index,) + span])
                coup[span] = coup[span] + jnp.where(alive, term, 0.0)
        return carry

    lax.fori_loop(0, degree, first_body, 0)

    def up(vector, write):
        def body(band, carry):
            out = []
            for index in range(8):
                product = pre[band * 8 + index].astype(F32) * vector
                out.append(jnp.sum(product, axis=0, keepdims=True))
            write(pl.ds(pl.multiple_of(band * 8, 8), 8), jnp.concatenate(out, axis=0))
            return carry

        lax.fori_loop(0, rows // 8, body, 0)

    empty = jnp.zeros((rows, block), F32)
    for turn in range(ITERS):
        more = turn + 1 < ITERS
        coup[...] = coup[...] - KAPPA * finish_platoon(turn)
        rhs[...] = down(pre, coup, q[...])
        plan[...] = -down(inv, rhs, empty)

        def write_first(span, value):
            traj[turn + 1, span, :] = value + traj[0, span, :]

        up(plan[...], write_first)
        if turn > 0:
            factor = finish_peak(turn - 1)
            traj[turn + 1] = traj[turn + 1] + factor * slope[...]
        if ORDER == 0:
            start_near(turn + 1)
        if ORDER == 2:
            start_near(turn + 1, (-2, 2))
        if more:
            start_platoon(turn + 1)
        if ORDER == 1:
            start_near(turn + 1)
        if ORDER == 2:
            start_near(turn + 1, (-1, 1))
        if not more and turn > 0:
            plan[...] = plan[...] + factor * plan_slope[...]
        if more:
            middle_platoon(turn + 1)
        wait_near(turn + 1)
        coup[...] = jnp.zeros_like(coup)
        miss_sum[...] = jnp.zeros_like(miss_sum)

        def body(index, peak):
            for half in range(halves):
                alive, near = look(turn + 1, index, half)
                for band in range(rows // 8):
                    span = (pl.ds(band * 8, 8), pl.ds(half * LANES, LANES))
                    wish = near[band] + off[(index,) + span]
                    miss = jnp.where(alive, traj[(turn + 1,) + span] - wish, 0.0)
                    held = lam[(index,) + span]
                    if turn > 0:
                        held = held + gap[(index,) + span] * factor
                        lam[(index,) + span] = held
                    gap[(index,) + span] = miss
                    peak = jnp.maximum(peak, jnp.abs(miss))
                    if more:
                        term = held - RHO * wish
                        coup[span] = coup[span] + jnp.where(alive, term, 0.0)
                        miss_sum[span] = miss_sum[span] + miss
            return peak

        peak = lax.fori_loop(0, degree, body, jnp.zeros((8, LANES), F32))
        start_peak(turn, peak)
        if more:
            late_platoon(turn + 1)
            rhs[...] = down(pre, miss_sum, empty)
            plan_slope[...] = -down(inv, rhs, empty)

            def write_slope(span, value):
                slope[span, :] = value

            up(plan_slope[...], write_slope)

    scale[...] = jnp.broadcast_to(finish_peak(ITERS - 1), scale.shape)


def finish(plan, lam, gap, scale, plan_hbm, lam_hbm, buffer, sems):
    copies = [pltpu.make_async_copy(plan, plan_hbm, sems.at[0])]
    copies[0].start()
    for index in range(lam.shape[0]):
        buffer[index] = lam[index] + gap[index] * scale[...]
        copies.append(pltpu.make_async_copy(buffer.at[index], lam_hbm.at[index], sems.at[1 + index]))
        copies[-1].start()
    for copy in copies:
        copy.wait()


def local(agents, group, q_lin, inverse, predict, free_traj, offsets, multipliers, nbr_owner, nbr_slot, platoon):
    rows, block = q_lin.shape[1:]
    degree = nbr_slot.shape[1]
    fold = 2 if agents % 2 == 0 else 1
    lines, plane = agents // fold, fold * group
    part = -(-rows // plane)
    tile = (-(-(part + 1) // 8) * 8, NPLAT)
    turns = ITERS
    wide = 2 * SPAN + 1
    dma = lambda *shape: pltpu.SemaphoreType.DMA(shape)
    vmem = lambda *shape: pltpu.VMEM(shape, F32)
    anywhere = pl.BlockSpec(memory_space=pl.ANY)
    whole = pl.BlockSpec(memory_space=pltpu.VMEM)
    plan, lam, gap, scale = pl.pallas_call(
        functools.partial(kernel, agents, group, fold),
        out_shape=(
            pltpu.VMEM((rows, block), F32),
            pltpu.VMEM((degree, rows, block), F32),
            pltpu.VMEM((degree, rows, block), F32),
            pltpu.VMEM((1, block), F32),
        ),
        in_specs=[anywhere] * 9,
        out_specs=[whole] * 4,
        scratch_shapes=[
            vmem(rows, block),
            pltpu.VMEM((rows, rows, block), BF16),
            pltpu.VMEM((rows, rows, block), BF16),
            vmem(degree, rows, block),
            pltpu.VMEM((degree, block), jnp.int32),
            pltpu.VMEM((degree, block), jnp.int32),
            pltpu.VMEM((1, block), jnp.int32),
            vmem(rows, block),
            vmem(rows, block),
            vmem(rows, block),
            vmem(rows, block),
            vmem(rows, block),
            vmem(turns + 1, rows, block),
            vmem(turns + 1, wide, rows, block),
            vmem(turns, plane, *tile),
            vmem(turns, plane, *tile),
            vmem(turns, *tile),
            vmem(turns, lines, *tile),
            vmem(turns, *tile),
            vmem(turns, plane, *tile),
            vmem(turns, 1, LANES),
            vmem(turns, agents * group, 1, LANES),
            vmem(1, NPLAT),
            pltpu.VMEM((degree, 8, block), jnp.int32),
            pltpu.VMEM((degree, 8, block), jnp.int32),
            dma(9),
            dma(turns + 1, wide), dma(turns + 1, wide),
            dma(turns, plane), dma(turns, plane),
            dma(turns, lines), dma(turns, lines),
            dma(turns, plane), dma(turns, plane),
            dma(turns), dma(turns),
        ],
        compiler_params=pltpu.CompilerParams(collective_id=0, has_side_effects=True),
    )(
        q_lin[0], inverse[0], predict[0], free_traj[0], offsets[0], multipliers[0],
        nbr_owner[0], nbr_slot[0], platoon,
    )
    plan, lam = pl.pallas_call(
        finish,
        out_shape=(
            jax.ShapeDtypeStruct((rows, block), F32),
            jax.ShapeDtypeStruct((degree, rows, block), F32),
        ),
        in_specs=[whole] * 4,
        out_specs=[anywhere] * 2,
        scratch_shapes=[vmem(degree, rows, block), dma(degree + 1)],
    )(*(pltpu.with_memory_space_constraint(x, pltpu.VMEM) for x in (plan, lam, gap, scale)))
    return plan[None], lam[None]


def solution(mesh):
    agents, group = mesh.shape["agents"], mesh.shape["group"]
    return jax.shard_map(
        functools.partial(local, agents, group),
        mesh=mesh,
        in_specs=(
            P("group", None, "agents"),
            P("group", None, None, "agents"),
            P("group", None, None, "agents"),
            P("group", None, "agents"),
            P("group", None, None, "agents"),
            P("group", None, None, "agents"),
            P("group", None, "agents"),
            P("group", None, "agents"),
            P("group", "agents"),
        ),
        out_specs=(P("group", None, "agents"), P("group", None, None, "agents")),
        check_vma=False,
    )
```

```python
import functools

import jax
import jax.numpy as jnp
from jax import lax
from jax.experimental import pallas as pl
from jax.experimental.pallas import tpu as pltpu
from jax.sharding import PartitionSpec as P

SPAN = 2
NPLAT = 128
ITERS = 3
RHO = 0.5
KAPPA = 0.5
LANES = 128
F32 = jnp.float32
BF16 = jnp.bfloat16
ORDER = 2
MESH = pl.DeviceIdType.MESH


def split(value):
    high = value.astype(BF16)
    low = (value - high.astype(F32)).astype(BF16)
    return high, low


def kernel(
    agents, group, fold,
    q_hbm, inv_hbm, pre_hbm, free_hbm, off_hbm, mul_hbm, owner_hbm, slot_hbm, plat_hbm,
    plan, lam, gap, scale,
    q, inv, pre, off, owner, slot, plat,
    coup, rhs, miss_sum, slope, plan_slope, traj, near_in,
    rs_out, rs_in, line_out, line_in, ag_out, ag_in, peak_out, peak_in,
    inv_count, lane_tab, tile_tab,
    load_sem,
    near_send, near_recv, rs_send, rs_recv, line_send, line_recv, ag_send, ag_recv,
    peak_send, peak_recv,
):
    me = lax.axis_index("agents")
    mine = lax.axis_index("group")
    lines = agents // fold
    plane = fold * group
    everyone = agents * group
    high, low = me // fold, me % fold
    spot = low * group + mine
    rows, block = q.shape
    degree = slot.shape[0]
    halves = block // LANES
    part = -(-rows // plane)

    loads = {}
    for number, (name, source, target) in enumerate((
        ("free", free_hbm, traj.at[0]), ("plat", plat_hbm, plat), ("slot", slot_hbm, slot),
        ("owner", owner_hbm, owner), ("q", q_hbm, q), ("lam", mul_hbm, lam), ("off", off_hbm, off),
        ("pre", pre_hbm, pre), ("inv", inv_hbm, inv),
    )):
        loads[name] = pltpu.make_async_copy(source, target, load_sem.at[number])
        loads[name].start()

    def plane_peer(offset):
        other = lax.rem(spot + offset, plane)
        return other, {"agents": high * fold + other // group, "group": lax.rem(other, group)}

    def line_peer(offset):
        return {"agents": lax.rem(high + offset, lines) * fold + low, "group": mine}

    def exists(step):
        return jnp.logical_and(me + step >= 0, me + step < agents)

    steps = [d for d in range(-SPAN, SPAN + 1) if d != 0]
    barrier = pltpu.get_barrier_semaphore()
    for offset in range(1, plane):
        pl.semaphore_signal(barrier, inc=1, device_id=plane_peer(offset)[1], device_id_type=MESH)
    for offset in range(1, lines):
        pl.semaphore_signal(barrier, inc=1, device_id=line_peer(offset), device_id_type=MESH)
    expected = plane - 1 + lines - 1
    for step in steps:
        @pl.when(exists(step))
        def _():
            pl.semaphore_signal(
                barrier, inc=1, device_id={"agents": me + step, "group": mine}, device_id_type=MESH
            )
        expected = expected + jnp.where(exists(step), 1, 0)

    def near_copy(turn, step):
        return pltpu.make_async_remote_copy(
            src_ref=traj.at[turn], dst_ref=near_in.at[turn, SPAN - step],
            send_sem=near_send.at[turn, SPAN + step], recv_sem=near_recv.at[turn, SPAN - step],
            device_id={"agents": me + step, "group": mine}, device_id_type=MESH)

    def near_arrival(turn, step):
        return pltpu.make_async_remote_copy(
            src_ref=traj.at[turn], dst_ref=near_in.at[turn, SPAN + step],
            send_sem=near_send.at[turn, SPAN + step], recv_sem=near_recv.at[turn, SPAN + step],
            device_id={"agents": me + step, "group": mine}, device_id_type=MESH)

    def rs_copy(turn, offset):
        other, device = plane_peer(offset)
        return pltpu.make_async_remote_copy(
            src_ref=rs_out.at[turn, other], dst_ref=rs_in.at[turn, offset],
            send_sem=rs_send.at[turn, offset], recv_sem=rs_recv.at[turn, offset],
            device_id=device, device_id_type=MESH)

    def line_copy(turn, offset):
        return pltpu.make_async_remote_copy(
            src_ref=line_out.at[turn], dst_ref=line_in.at[turn, offset],
            send_sem=line_send.at[turn, offset], recv_sem=line_recv.at[turn, offset],
            device_id=line_peer(offset), device_id_type=MESH)

    def ag_copy(turn, offset):
        return pltpu.make_async_remote_copy(
            src_ref=ag_out.at[turn], dst_ref=ag_in.at[turn, spot],
            send_sem=ag_send.at[turn, offset], recv_sem=ag_recv.at[turn, offset],
            device_id=plane_peer(offset)[1], device_id_type=MESH)

    def ag_arrival(turn, offset):
        return pltpu.make_async_remote_copy(
            src_ref=ag_out.at[turn], dst_ref=ag_in.at[turn, lax.rem(spot + plane - offset, plane)],
            send_sem=ag_send.at[turn, offset], recv_sem=ag_recv.at[turn, offset],
            device_id=plane_peer(offset)[1], device_id_type=MESH)

    def peak_copy(turn, offset):
        other = lax.rem(me * group + mine + offset, everyone)
        return pltpu.make_async_remote_copy(
            src_ref=peak_out.at[turn], dst_ref=peak_in.at[turn, offset],
            send_sem=peak_send.at[turn], recv_sem=peak_recv.at[turn],
            device_id={"agents": other // group, "group": lax.rem(other, group)},
            device_id_type=MESH)

    def onehot():
        names = lax.broadcasted_iota(jnp.int32, (NPLAT, block), 0)
        return jnp.where(names == plat[...], 1.0, 0.0).astype(BF16)

    def platoon_sums(value):
        hot = onehot()
        dims = (((1,), (1,)), ((), ()))
        first, second = split(value)
        return lax.dot_general(first, hot, dims, preferred_element_type=F32) + lax.dot_general(
            second, hot, dims, preferred_element_type=F32)

    def store_sums(turn):
        sums = platoon_sums(traj[turn])
        for piece in range(plane):
            begin, end = min(rows, piece * part), min(rows, (piece + 1) * part)
            if end > begin:
                rs_out[turn, piece, 0:end - begin, :] = sums[begin:end, :]
            if turn == 0:
                ones = jnp.ones((16, block), BF16)
                if piece == 0:
                    counts = lax.dot_general(
                        ones, onehot(), (((1,), (1,)), ((), ())), preferred_element_type=F32)[0:1]
                rs_out[turn, piece, part:part + 1, :] = counts

    def send_sums(turn):
        for offset in range(1, plane):
            rs_copy(turn, offset).start()

    def start_platoon(turn):
        store_sums(turn)
        send_sums(turn)

    def middle_platoon(turn):
        total = rs_out[turn, spot]
        for offset in range(1, plane):
            rs_copy(turn, offset).wait()
            total = total + rs_in[turn, offset]
        line_out[turn] = total
        for offset in range(1, lines):
            line_copy(turn, offset).start()

    def late_platoon(turn):
        total = line_out[turn]
        for offset in range(1, lines):
            line_copy(turn, offset).wait()
            total = total + line_in[turn, offset]
        if turn == 0:
            inv_count[...] = 1.0 / jnp.maximum(total[part:part + 1, :], 1.0)
        mean = total * inv_count[...]
        ag_out[turn] = mean
        for offset in range(1, plane):
            ag_copy(turn, offset).start()
        ag_in[turn, spot] = mean

    def finish_platoon(turn):
        for offset in range(1, plane):
            ag_copy(turn, offset).wait_send()
            ag_arrival(turn, offset).wait_recv()
        pieces = []
        for piece in range(plane):
            begin, end = min(rows, piece * part), min(rows, (piece + 1) * part)
            if end > begin:
                pieces.append(ag_in[turn, piece, 0:end - begin, :])
        means = jnp.concatenate(pieces, axis=0)
        hot = onehot()
        first, second = split(means)
        return jnp.dot(first, hot, preferred_element_type=F32) + jnp.dot(
            second, hot, preferred_element_type=F32)

    def start_near(turn, steps=steps):
        for step in steps:
            @pl.when(exists(step))
            def _():
                near_copy(turn, step).start()

    def wait_near(turn):
        for step in steps:
            @pl.when(exists(step))
            def _():
                near_copy(turn, step).wait_send()
                near_arrival(turn, step).wait_recv()

    def look(turn, slot_index, half):
        window = pl.ds(half * LANES, LANES)
        lane = lane_tab[slot_index, :, window]
        tile = tile_tab[slot_index, :, window]
        out = []
        for band in range(rows // 8):
            near = jnp.zeros((8, LANES), F32)
            for distance in range(2 * SPAN + 1):
                for side in range(halves):
                    span = (pl.ds(band * 8, 8), pl.ds(side * LANES, LANES))
                    if distance == SPAN:
                        source = traj[(turn,) + span]
                    else:
                        source = near_in[(turn, distance) + span]
                    taken = jnp.take_along_axis(source, lane, axis=1, mode="promise_in_bounds")
                    near = jnp.where(tile == distance * halves + side, taken, near)
            out.append(near)
        return tile >= 0, out

    def start_peak(turn, peak):
        peak_out[turn] = jnp.max(peak, axis=0, keepdims=True)
        for offset in range(1, everyone):
            peak_copy(turn, offset).start()

    def finish_peak(turn):
        landed = peak_in.at[turn, pl.ds(1, everyone - 1)]
        pltpu.make_async_copy(landed, landed, peak_send.at[turn]).wait()
        pltpu.make_async_copy(landed, landed, peak_recv.at[turn]).wait()
        peak = peak_out[turn]
        for offset in range(1, everyone):
            peak = jnp.maximum(peak, peak_in[turn, offset])
        return 1.0 / (1.0 + jnp.max(peak, axis=1, keepdims=True))

    def tables():
        where = slot[...]
        tile = jnp.where(where >= 0, (owner[...] - me + SPAN) * halves + where // LANES, -1)
        lane = lax.rem(jnp.maximum(where, 0), LANES)
        for index in range(degree):
            lane_tab[index] = jnp.broadcast_to(lane[index:index + 1], (8, block))
            tile_tab[index] = jnp.broadcast_to(tile[index:index + 1], (8, block))

    def down(matrix, vector_ref, start):
        def body(band, total):
            rows8 = vector_ref[pl.ds(pl.multiple_of(band * 8, 8), 8), :]
            for index in range(8):
                total = total + matrix[band * 8 + index].astype(F32) * rows8[index:index + 1, :]
            return total
        return lax.fori_loop(0, rows // 8, body, start)

    loads["free"].wait()
    loads["plat"].wait()
    rs_out[...] = jnp.zeros_like(rs_out)
    store_sums(0)
    pl.semaphore_wait(barrier, expected)
    send_sums(0)
    start_near(0)
    for name in ("slot", "owner", "q", "lam", "off", "pre", "inv"):
        loads[name].wait()
    tables()
    middle_platoon(0)
    wait_near(0)
    late_platoon(0)

    coup[...] = jnp.zeros_like(coup)

    def first_body(index, carry):
        for half in range(halves):
            alive, near = look(0, index, half)
            for band in range(rows // 8):
                span = (pl.ds(band * 8, 8), pl.ds(half * LANES, LANES))
                term = lam[(index,) + span] - RHO * (near[band] + off[(index,) + span])
                coup[span] = coup[span] + jnp.where(alive, term, 0.0)
        return carry

    lax.fori_loop(0, degree, first_body, 0)

    def up(vector, write):
        def body(band, carry):
            out = []
            for index in range(8):
                product = pre[band * 8 + index].astype(F32) * vector
                out.append(jnp.sum(product, axis=0, keepdims=True))
            write(pl.ds(pl.multiple_of(band * 8, 8), 8), jnp.concatenate(out, axis=0))
            return carry

        lax.fori_loop(0, rows // 8, body, 0)

    empty = jnp.zeros((rows, block), F32)
    for turn in range(ITERS):
        more = turn + 1 < ITERS
        coup[...] = coup[...] - KAPPA * finish_platoon(turn)
        rhs[...] = down(pre, coup, q[...])
        plan[...] = -down(inv, rhs, empty)

        def write_first(span, value):
            traj[turn + 1, span, :] = value + traj[0, span, :]

        up(plan[...], write_first)
        if turn > 0:
            factor = finish_peak(turn - 1)
            traj[turn + 1] = traj[turn + 1] + factor * slope[...]
        if ORDER == 0:
            start_near(turn + 1)
        if ORDER == 2:
            start_near(turn + 1, (-2, 2))
        if more:
            start_platoon(turn + 1)
        if ORDER == 1:
            start_near(turn + 1)
        if ORDER == 2:
            start_near(turn + 1, (-1, 1))
        if not more and turn > 0:
            plan[...] = plan[...] + factor * plan_slope[...]
        if more:
            middle_platoon(turn + 1)
        wait_near(turn + 1)
        coup[...] = jnp.zeros_like(coup)
        miss_sum[...] = jnp.zeros_like(miss_sum)

        def body(index, peak):
            for half in range(halves):
                alive, near = look(turn + 1, index, half)
                for band in range(rows // 8):
                    span = (pl.ds(band * 8, 8), pl.ds(half * LANES, LANES))
                    wish = near[band] + off[(index,) + span]
                    miss = jnp.where(alive, traj[(turn + 1,) + span] - wish, 0.0)
                    held = lam[(index,) + span]
                    if turn > 0:
                        held = held + gap[(index,) + span] * factor
                        lam[(index,) + span] = held
                    gap[(index,) + span] = miss
                    peak = jnp.maximum(peak, jnp.abs(miss))
                    if more:
                        term = held - RHO * wish
                        coup[span] = coup[span] + jnp.where(alive, term, 0.0)
                        miss_sum[span] = miss_sum[span] + miss
            return peak

        peak = lax.fori_loop(0, degree, body, jnp.zeros((8, LANES), F32))
        start_peak(turn, peak)
        if more:
            late_platoon(turn + 1)
            rhs[...] = down(pre, miss_sum, empty)
            plan_slope[...] = -down(inv, rhs, empty)

            def write_slope(span, value):
                slope[span, :] = value

            up(plan_slope[...], write_slope)

    scale[...] = jnp.broadcast_to(finish_peak(ITERS - 1), scale.shape)


def finish(plan, lam, gap, scale, plan_hbm, lam_hbm, buffer, sems):
    copies = [pltpu.make_async_copy(plan, plan_hbm, sems.at[0])]
    copies[0].start()
    for index in range(lam.shape[0]):
        buffer[index] = lam[index] + gap[index] * scale[...]
        copies.append(pltpu.make_async_copy(buffer.at[index], lam_hbm.at[index], sems.at[1 + index]))
        copies[-1].start()
    for copy in copies:
        copy.wait()


def local(agents, group, q_lin, inverse, predict, free_traj, offsets, multipliers, nbr_owner, nbr_slot, platoon):
    rows, block = q_lin.shape[1:]
    degree = nbr_slot.shape[1]
    fold = 1
    lines, plane = agents // fold, fold * group
    part = -(-rows // plane)
    tile = (part + 1, NPLAT)
    turns = ITERS
    wide = 2 * SPAN + 1
    dma = lambda *shape: pltpu.SemaphoreType.DMA(shape)
    vmem = lambda *shape: pltpu.VMEM(shape, F32)
    anywhere = pl.BlockSpec(memory_space=pl.ANY)
    whole = pl.BlockSpec(memory_space=pltpu.VMEM)
    plan, lam, gap, scale = pl.pallas_call(
        functools.partial(kernel, agents, group, fold),
        out_shape=(
            pltpu.VMEM((rows, block), F32),
            pltpu.VMEM((degree, rows, block), F32),
            pltpu.VMEM((degree, rows, block), F32),
            pltpu.VMEM((1, block), F32),
        ),
        in_specs=[anywhere] * 9,
        out_specs=[whole] * 4,
        scratch_shapes=[
            vmem(rows, block),
            pltpu.VMEM((rows, rows, block), BF16),
            pltpu.VMEM((rows, rows, block), BF16),
            vmem(degree, rows, block),
            pltpu.VMEM((degree, block), jnp.int32),
            pltpu.VMEM((degree, block), jnp.int32),
            pltpu.VMEM((1, block), jnp.int32),
            vmem(rows, block),
            vmem(rows, block),
            vmem(rows, block),
            vmem(rows, block),
            vmem(rows, block),
            vmem(turns + 1, rows, block),
            vmem(turns + 1, wide, rows, block),
            vmem(turns, plane, *tile),
            vmem(turns, plane, *tile),
            vmem(turns, *tile),
            vmem(turns, lines, *tile),
            vmem(turns, *tile),
            vmem(turns, plane, *tile),
            vmem(turns, 1, LANES),
            vmem(turns, agents * group, 1, LANES),
            vmem(1, NPLAT),
            pltpu.VMEM((degree, 8, block), jnp.int32),
            pltpu.VMEM((degree, 8, block), jnp.int32),
            dma(9),
            dma(turns + 1, wide), dma(turns + 1, wide),
            dma(turns, plane), dma(turns, plane),
            dma(turns, lines), dma(turns, lines),
            dma(turns, plane), dma(turns, plane),
            dma(turns), dma(turns),
        ],
        compiler_params=pltpu.CompilerParams(collective_id=0, has_side_effects=True),
    )(
        q_lin[0], inverse[0], predict[0], free_traj[0], offsets[0], multipliers[0],
        nbr_owner[0], nbr_slot[0], platoon,
    )
    plan, lam = pl.pallas_call(
        finish,
        out_shape=(
            jax.ShapeDtypeStruct((rows, block), F32),
            jax.ShapeDtypeStruct((degree, rows, block), F32),
        ),
        in_specs=[whole] * 4,
        out_specs=[anywhere] * 2,
        scratch_shapes=[vmem(degree, rows, block), dma(degree + 1)],
    )(*(pltpu.with_memory_space_constraint(x, pltpu.VMEM) for x in (plan, lam, gap, scale)))
    return plan[None], lam[None]


def solution(mesh):
    agents, group = mesh.shape["agents"], mesh.shape["group"]
    return jax.shard_map(
        functools.partial(local, agents, group),
        mesh=mesh,
        in_specs=(
            P("group", None, "agents"),
            P("group", None, None, "agents"),
            P("group", None, None, "agents"),
            P("group", None, "agents"),
            P("group", None, None, "agents"),
            P("group", None, None, "agents"),
            P("group", None, "agents"),
            P("group", None, "agents"),
            P("group", "agents"),
        ),
        out_specs=(P("group", None, "agents"), P("group", None, None, "agents")),
        check_vma=False,
    )
```
